32 devices in a mesh: mesh: 8 (over z, x), field: 4 (over y, core).
Axes of the slice: x: 2, y: 2, z: 4, core: 2. Of those that a mesh axis runs over, the one named last changes fastest.
Arguments:
- velocity: float32 [3, 32, 1024], P(None, ('mesh', 'field')), may hold values from -4 to 4
- pressure: float32 [32, 1024], P(('mesh', 'field')), may hold values from -128 to 128
- fields: bfloat16 [3, 256, 32, 1024], P(None, 'field', 'mesh'), may hold values from -1.8 to 1.8
- brownian: bfloat16 [3, 256, 32, 1024], P(None, 'field', 'mesh'), may hold values from -4 to 4
Outputs:
- new_fields: bfloat16 [3, 256, 32, 1024], P(None, 'field', 'mesh')
- new_velocity: float32 [3, 32, 1024], P(None, ('mesh', 'field'))
The draws below stay inside these ranges and needn't reach their ends.
All inputs are finite; a program needn't handle non-finite values.
Results may differ from the reference program's by a relative error of at most 0.001.
Values sent between devices are 32-bit elements; how exact they have to be, the bound alone decides.
A program may use at most 64 MiB of HBM per device.

```python
import math
import jax
import jax.numpy as jnp
from jax import lax

NF = 256
NY = 32
NZ = 32
CXF = 1
SWEEPS = 4
PLANE = 1024
NX = 32


def draw_fields(key, part):
    scale_key, value_key = jax.random.split(jax.random.fold_in(key, 7), 2)
    log_scale = jax.random.uniform(scale_key, (3, 1, NX, PLANE), jnp.float32, math.log(0.3), math.log(1.75))
    node_scale = jnp.exp(log_scale)
    values = jax.random.uniform(value_key, (3, NF, NX, PLANE), jnp.float32, -1.0, 1.0)
    return (node_scale * values).astype(jnp.bfloat16)


def block_scale(rng, shape, cuts, low, high):
    def one(dim, shards_of):
        heights = jax.random.uniform(jax.random.fold_in(jax.random.fold_in(rng, 6), dim), (shards_of,), jnp.float32, low / len(cuts), high / len(cuts))
        return jnp.repeat(jnp.exp(heights), shape[dim] // shards_of).reshape((-1,) + (1,) * (len(shape) - dim - 1))

    gain = one(*cuts[0])
    for cut in cuts[1:]:
        gain = gain * one(*cut)
    return gain


def bell_draw(stream_key, shape, width, limit, cuts=(), kind=jnp.bfloat16):
    level = block_scale(stream_key, shape, cuts, -0.22, 0.18) if cuts else 1.0
    values = jax.random.normal(stream_key, shape, jnp.float32) * width * level
    return jnp.minimum(jnp.maximum(values, -limit), limit).astype(kind)


def setup_inputs(seed: int = 0) -> dict:
    arg_keys = jax.random.split(jax.random.key(seed), 5)
    velocity = bell_draw(arg_keys[0], (3, NX, PLANE), 1.0, 4.0, ((1, 32),), jnp.float32)
    pressure = bell_draw(arg_keys[1], (NX, PLANE), 32.0, 128.0, ((0, 32),), jnp.float32)
    fields = draw_fields(jax.random.fold_in(arg_keys[4], 71), 0)
    brownian = bell_draw(arg_keys[3], (3, NF, NX, PLANE), 1.0, 4.0, ((1, 4), (2, 8)))
    return {"velocity": velocity, "pressure": pressure, "fields": fields, "brownian": brownian}


time_step = 0.02
axial_weight = 400.0
transverse_weight = 40.0
weissenberg = 0.5
max_stretch = 50.0
polymer_viscosity = 40.0
noise_scale = (0.02 / 0.5) ** 0.5
diagonal_weight = 1.0 / 0.02 + 2.0 * 400.0 + 4.0 * 40.0
index_table = ((0, 1, 2), (1, 3, 4), (2, 4, 5))
component_pairs = ((0, 0), (0, 1), (0, 2), (1, 1), (1, 2), (2, 2))


def plane_shifts(values):
    extent = values.shape[-1]
    leading = [(0, 0)] * (values.ndim - 1)
    along_y = jnp.pad(values, leading + [(NZ, NZ)])
    along_z = jnp.pad(values, leading + [(1, 1)])
    column = lax.broadcasted_iota(jnp.int32, (extent,), 0) % NZ
    upper_keep = (column < NZ - 1).astype(values.dtype)
    lower_keep = (column > 0).astype(values.dtype)
    return along_y[..., 2 * NZ:], along_y[..., :extent], along_z[..., 2:] * upper_keep, along_z[..., :extent] * lower_keep


def derivatives(padded):
    interior = padded[:, 1:-1]
    y_plus, y_minus, z_plus, z_minus = plane_shifts(interior)
    return ((padded[:, 2:] - padded[:, :-2]) * 0.5, (y_plus - y_minus) * 0.5, (z_plus - z_minus) * 0.5)


def velocity_gradient(padded):
    stacked = jnp.stack(derivatives(padded), axis=1)
    return stacked.reshape(9, stacked.shape[2], stacked.shape[3])


def advance(fields, brownian, gradient):
    current = fields.astype(jnp.float32)
    increments = brownian.astype(jnp.float32)
    length_sq = current[0] * current[0] + current[1] * current[1] + current[2] * current[2]
    spring = 1.0 / (1.0 - length_sq / max_stretch)
    drift_terms = []
    for out_axis in range(3):
        stretch = gradient[3 * out_axis][None] * current[0] + gradient[3 * out_axis + 1][None] * current[1] + gradient[3 * out_axis + 2][None] * current[2]
        drift_terms.append(stretch - spring * current[out_axis] / (2.0 * weissenberg))
    advanced = current + time_step * jnp.stack(drift_terms) + noise_scale * increments
    new_sq = advanced[0] * advanced[0] + advanced[1] * advanced[1] + advanced[2] * advanced[2]
    new_spring = 1.0 / (1.0 - new_sq / max_stretch)
    partial_value = jnp.stack([jnp.sum(new_spring * advanced[left_axis] * advanced[right_axis], axis=0) for left_axis, right_axis in component_pairs])
    return advanced.astype(jnp.bfloat16), partial_value


def to_stress(summed):
    identity = jnp.array([1.0, 0.0, 0.0, 1.0, 0.0, 1.0], dtype=summed.dtype)[:, None, None]
    return (polymer_viscosity / weissenberg) * (summed / NF - identity)


def momentum_source(velocity, padded_pressure, padded_stress):
    pressure_grad = jnp.concatenate(derivatives(padded_pressure), axis=0)
    slopes = derivatives(padded_stress)
    divergence = jnp.stack([slopes[0][index_table[out_axis][0]] + slopes[1][index_table[out_axis][1]] + slopes[2][index_table[out_axis][2]] for out_axis in range(3)])
    return velocity / time_step - pressure_grad + divergence


def fluid_mask(offset, planes, total_planes, extent):
    position = offset + lax.broadcasted_iota(jnp.int32, (planes, extent), 0)
    across = lax.broadcasted_iota(jnp.int32, (planes, extent), 1) // NZ
    blocked = (position >= total_planes // 2) & ((across < NY // 4) | (across >= NY - NY // 4))
    return jnp.where(blocked, 0.0, 1.0).astype(jnp.float32)


def relax_step(padded, source, fluid):
    interior = padded[:, 1:-1]
    y_plus, y_minus, z_plus, z_minus = plane_shifts(interior)
    along_flow = padded[:, 2:] + padded[:, :-2]
    across_flow = y_plus + y_minus + z_plus + z_minus
    return fluid * (source + axial_weight * along_flow + transverse_weight * across_flow) / diagonal_weight


def reference(velocity, pressure, fields, brownian):
    stacked = jnp.concatenate([velocity, pressure[None]], axis=0)
    padded = jnp.pad(stacked, ((0, 0), (1, 1), (0, 0)))
    gradient = velocity_gradient(padded[:3])

    def one_block(number):
        first_plane = (number * CXF).astype(jnp.int32)
        return advance(lax.dynamic_slice_in_dim(fields, first_plane, CXF, 2),
                       lax.dynamic_slice_in_dim(brownian, first_plane, CXF, 2),
                       lax.dynamic_slice_in_dim(gradient, first_plane, CXF, 1))

    advanced, partial_value = lax.map(one_block, jnp.arange(NX // CXF, dtype=jnp.int32))
    new_fields = jnp.moveaxis(advanced, 0, 2).reshape(3, NF, NX, PLANE)
    summed = jnp.moveaxis(partial_value, 0, 1).reshape(6, NX, PLANE)
    stress = to_stress(summed)
    padded_stress = jnp.pad(stress, ((0, 0), (1, 1), (0, 0)))
    source = momentum_source(velocity, padded[3:], padded_stress)
    fluid = fluid_mask(0, NX, NX, PLANE)
    current = velocity
    for repeat in range(SWEEPS):
        current = relax_step(jnp.pad(current, ((0, 0), (1, 1), (0, 0))), source, fluid)
    return new_fields, current
```

```python
import functools

import jax
import jax.numpy as jnp
from jax import lax
from jax.experimental import pallas as pl
from jax.experimental.pallas import tpu as pltpu
from jax.sharding import PartitionSpec as P

NY = 32
NZ = 32
SWEEPS = 4
LANES = 128
CHUNKS = 4

time_step = 0.02
axial_weight = 400.0
transverse_weight = 40.0
weissenberg = 0.5
max_stretch = 50.0
polymer_viscosity = 40.0
noise_scale = (0.02 / 0.5) ** 0.5
diagonal_weight = 1.0 / 0.02 + 2.0 * 400.0 + 4.0 * 40.0
index_table = ((0, 1, 2), (1, 3, 4), (2, 4, 5))
component_pairs = ((0, 0), (0, 1), (0, 2), (1, 1), (1, 2), (2, 2))
diagonal_pairs = (0, 3, 5)


def plane_shifts(x):
    rows = x.shape[0]
    lane = lax.broadcasted_iota(jnp.int32, x.shape, 1)
    row = lax.broadcasted_iota(jnp.int32, x.shape, 0)
    column = lane % NZ
    ahead = pltpu.roll(x, LANES - NZ, 1)
    ahead_next = jnp.where(row == rows - 1, 0.0, pltpu.roll(ahead, rows - 1, 0))
    y_plus = jnp.where(lane >= LANES - NZ, ahead_next, ahead)
    behind = pltpu.roll(x, NZ, 1)
    behind_next = jnp.where(row == 0, 0.0, pltpu.roll(behind, 1, 0))
    y_minus = jnp.where(lane < NZ, behind_next, behind)
    z_plus = jnp.where(column < NZ - 1, pltpu.roll(x, LANES - 1, 1), 0.0)
    z_minus = jnp.where(column > 0, pltpu.roll(x, 1, 1), 0.0)
    return y_plus, y_minus, z_plus, z_minus


def step_kernel(
    subdomains, groups,
    vel, prs, fld, brn, out_fields, out_vel,
    cur, noise, base, advanced, grads, sums, vp, parts, got, stress, vout,
    load_sem, flow_sem, vp_send, vp_recv, part_send, part_recv, st_send, st_recv, out_sem,
):
    total = subdomains * groups
    halo = SWEEPS
    width = max(halo, groups)
    rows = vel.shape[1]
    count = fld.shape[1]
    packed = fld.shape[2]
    block = min(16, packed)
    chunk = count // CHUNKS
    sub = lax.axis_index("mesh")
    own = lax.axis_index("field")
    plane = sub * groups + own
    offsets = [d for d in range(-width, width + 1) if d != 0]

    def inside(d):
        return (plane + d >= 0) & (plane + d < total)

    def device(d):
        return ((plane + d) // groups, (plane + d) % groups)

    flow_loads = [
        pltpu.make_async_copy(vel, vp.at[width, pl.ds(0, 3)], flow_sem.at[0]),
        pltpu.make_async_copy(prs, vp.at[width, 3], flow_sem.at[1]),
    ]
    for copy in flow_loads:
        copy.start()
    barrier = pltpu.get_barrier_semaphore()
    partners = jnp.int32(0)
    for d in offsets:
        @pl.when(inside(d))
        def _(d=d):
            pl.semaphore_signal(
                barrier, inc=1, device_id=device(d), device_id_type=pl.DeviceIdType.MESH
            )
        partners = partners + jnp.where(inside(d), 1, 0)
    loads = []
    for number in range(CHUNKS):
        part = pl.ds(number * chunk, chunk)
        loads.append((
            pltpu.make_async_copy(fld.at[:, part], cur.at[:, part], load_sem.at[0, number]),
            pltpu.make_async_copy(brn.at[:, part], noise.at[:, part], load_sem.at[1, number]),
        ))
        for copy in loads[-1]:
            copy.start()
    for d in offsets:
        @pl.when(jnp.logical_not(inside(d)))
        def _(d=d):
            vp[width + d] = jnp.zeros(vp.shape[1:], jnp.float32)
            stress[width + d] = jnp.zeros(stress.shape[1:], jnp.float32)
    for copy in flow_loads:
        copy.wait()
    pl.semaphore_wait(barrier, partners)

    def flow_copy(d):
        return pltpu.make_async_remote_copy(
            src_ref=vp.at[width], dst_ref=vp.at[width - d],
            send_sem=vp_send.at[width + d], recv_sem=vp_recv.at[width - d],
            device_id=device(d), device_id_type=pl.DeviceIdType.MESH,
        )

    for d in offsets:
        @pl.when(inside(d))
        def _(d=d):
            flow_copy(d).start()

    relax = time_step * max_stretch / (2.0 * weissenberg)
    for number in range(CHUNKS):
        for copy in loads[number]:
            copy.wait()

        @pl.loop(number * chunk, (number + 1) * chunk, unroll=2)
        def _(n):
            for start in range(0, packed, block):
                at = pl.ds(start, block)
                now = [cur[c, n, at].astype(jnp.float32) for c in range(3)]
                square = now[0] * now[0] + now[1] * now[1] + now[2] * now[2]
                keep = 1.0 - relax * (1.0 / (max_stretch - square))
                for c in range(3):
                    base[c, n, at] = now[c] * keep + noise_scale * noise[c, n, at].astype(jnp.float32)

    def wait_flow(slot):
        pltpu.make_async_copy(vp.at[width], vp.at[slot], vp_recv.at[slot]).wait()

    for q in range(-1, groups + 1):
        d = q - own
        @pl.when((d != 0) & inside(d))
        def _(d=d):
            wait_flow(width + d)
    for q in range(groups):
        here = width + q - own
        at = pl.ds(q, rows, stride=groups)
        for a in range(3):
            centre = vp[here, a]
            y_plus, y_minus, z_plus, z_minus = plane_shifts(centre)
            scale = 0.5 * time_step
            grads[3 * a, at] = (vp[here + 1, a] - vp[here - 1, a]) * scale
            grads[3 * a + 1, at] = (y_plus - y_minus) * scale
            grads[3 * a + 2, at] = (z_plus - z_minus) * scale

    writes = []
    for start in range(0, packed, block):
        at = pl.ds(start, block)
        g = [grads[k, at] for k in range(9)]

        def one_field(n, acc):
            now = [cur[c, n, at].astype(jnp.float32) for c in range(3)]
            new = []
            for a in range(3):
                value = base[a, n, at] + (
                    g[3 * a] * now[0] + g[3 * a + 1] * now[1] + g[3 * a + 2] * now[2]
                )
                advanced[a, n, at] = value.astype(jnp.bfloat16)
                new.append(value)
            square = new[0] * new[0] + new[1] * new[1] + new[2] * new[2]
            inverse = 1.0 / (max_stretch - square)
            pulled = [inverse * value for value in new]
            return tuple(
                total_k + pulled[left] * new[right]
                for total_k, (left, right) in zip(acc, component_pairs)
            )

        zero = jnp.zeros((block, LANES), jnp.float32)
        acc = lax.fori_loop(0, count, one_field, (zero,) * 6, unroll=2)
        for k in range(6):
            sums[k, at] = acc[k]
        writes.append(pltpu.make_async_copy(
            advanced.at[:, :, at], out_fields.at[:, :, at], out_sem.at[start // block]
        ))
        writes[-1].start()

    for q in range(groups):
        for k in range(6):
            parts[q, k] = sums[k, pl.ds(q, rows, stride=groups)]

    def part_copy(r):
        to = (own + r) % groups
        return pltpu.make_async_remote_copy(
            src_ref=parts.at[to], dst_ref=got.at[r - 1],
            send_sem=part_send.at[r - 1], recv_sem=part_recv.at[r - 1],
            device_id=(sub, to), device_id_type=pl.DeviceIdType.MESH,
        )

    for r in range(1, groups):
        part_copy(r).start()

    for d in offsets:
        q = own + d
        @pl.when(inside(d) & ((q < -1) | (q > groups)))
        def _(d=d):
            wait_flow(width + d)
    reach = halo - 1
    sources = {}
    fluid = {}
    across = (
        lax.broadcasted_iota(jnp.int32, (rows, LANES), 0) * (LANES // NZ)
        + lax.broadcasted_iota(jnp.int32, (rows, LANES), 1) // NZ
    )
    solid = jnp.where((across < NY // 4) | (across >= NY - NY // 4), 1.0, 0.0)
    for d in range(-reach, reach + 1):
        here = width + d
        y_plus, y_minus, z_plus, z_minus = plane_shifts(vp[here, 3])
        slopes = (vp[here + 1, 3] - vp[here - 1, 3], y_plus - y_minus, z_plus - z_minus)
        sources[d] = [vp[here, a] * (1.0 / time_step) - 0.5 * slopes[a] for a in range(3)]
        exists = jnp.where(inside(d), 1.0 / diagonal_weight, 0.0)
        narrow = jnp.where(plane + d >= total // 2, 1.0, 0.0)
        fluid[d] = exists * (1.0 - narrow * solid)

    for r in range(1, groups):
        part_copy(r).wait_recv()
    factor = polymer_viscosity / weissenberg
    for k in range(6):
        summed = parts[own, k]
        for r in range(1, groups):
            summed = summed + got[r - 1, k]
        value = summed * (factor * max_stretch / (count * groups))
        stress[width, k] = value - factor if k in diagonal_pairs else value

    def stress_copy(d):
        parts_of = pl.ds(0, 3 if abs(d) == halo else 6)
        return pltpu.make_async_remote_copy(
            src_ref=stress.at[width, parts_of], dst_ref=stress.at[width - d, parts_of],
            send_sem=st_send.at[width + d], recv_sem=st_recv.at[width - d],
            device_id=device(d), device_id_type=pl.DeviceIdType.MESH,
        )

    near = [d for d in offsets if abs(d) <= halo]
    for d in sorted(near, key=abs):
        @pl.when(inside(d))
        def _(d=d):
            stress_copy(d).start()
    for d in sorted(near, key=abs):
        @pl.when(inside(d))
        def _(d=d):
            stress_copy(-d).wait_recv()

    for d in range(-reach, reach + 1):
        here = width + d
        along_y = {}
        along_z = {}
        for k in range(1, 6):
            y_plus, y_minus, z_plus, z_minus = plane_shifts(stress[here, k])
            along_y[k] = y_plus - y_minus
            along_z[k] = z_plus - z_minus
        for a in range(3):
            along_x = stress[here + 1, a] - stress[here - 1, a]
            slope = along_x + along_y[index_table[a][1]] + along_z[index_table[a][2]]
            sources[d][a] = sources[d][a] + 0.5 * slope

    for a in range(3):
        v = {d: vp[width + d, a] for d in range(-halo, halo + 1)}
        for sweep in range(1, SWEEPS + 1):
            left = halo - sweep
            fresh = {}
            for d in range(-left, left + 1):
                y_plus, y_minus, z_plus, z_minus = plane_shifts(v[d])
                fresh[d] = fluid[d] * (
                    sources[d][a]
                    + axial_weight * (v[d + 1] + v[d - 1])
                    + transverse_weight * ((y_plus + y_minus) + (z_plus + z_minus))
                )
            v = fresh
        vout[a] = v[0]
    last = pltpu.make_async_copy(vout, out_vel, flow_sem.at[0])
    last.start()

    for d in offsets:
        @pl.when(inside(d))
        def _(d=d):
            flow_copy(d).wait_send()
            if abs(d) <= halo:
                stress_copy(d).wait_send()
    for r in range(1, groups):
        part_copy(r).wait_send()
    for copy in writes:
        copy.wait()
    last.wait()


def body(subdomains, groups, velocity, pressure, fields, brownian):
    extent = velocity.shape[2]
    count, depth = fields.shape[1], fields.shape[2]
    rows = extent // LANES
    packed = rows * depth
    width = max(SWEEPS, groups)

    def pack(values):
        split = values.reshape(3, count, depth, rows, LANES)
        return split.transpose(0, 1, 3, 2, 4).reshape(3, count, packed, LANES)

    dma = pltpu.SemaphoreType.DMA
    anywhere = pl.BlockSpec(memory_space=pl.ANY)
    new_fields, new_velocity = pl.pallas_call(
        functools.partial(step_kernel, subdomains, groups),
        out_shape=(
            jax.ShapeDtypeStruct((3, count, packed, LANES), jnp.bfloat16),
            jax.ShapeDtypeStruct((3, rows, LANES), jnp.float32),
        ),
        in_specs=[anywhere] * 4,
        out_specs=(anywhere, anywhere),
        scratch_shapes=[
            pltpu.VMEM((3, count, packed, LANES), jnp.bfloat16),
            pltpu.VMEM((3, count, packed, LANES), jnp.bfloat16),
            pltpu.VMEM((3, count, packed, LANES), jnp.float32),
            pltpu.VMEM((3, count, packed, LANES), jnp.bfloat16),
            pltpu.VMEM((9, packed, LANES), jnp.float32),
            pltpu.VMEM((6, packed, LANES), jnp.float32),
            pltpu.VMEM((2 * width + 1, 4, rows, LANES), jnp.float32),
            pltpu.VMEM((groups, 6, rows, LANES), jnp.float32),
            pltpu.VMEM((groups - 1, 6, rows, LANES), jnp.float32),
            pltpu.VMEM((2 * width + 1, 6, rows, LANES), jnp.float32),
            pltpu.VMEM((3, rows, LANES), jnp.float32),
            dma((2, CHUNKS)),
            dma((2,)),
            dma((2 * width + 1,)),
            dma((2 * width + 1,)),
            dma((groups - 1,)),
            dma((groups - 1,)),
            dma((2 * width + 1,)),
            dma((2 * width + 1,)),
            dma((packed // min(16, packed),)),
        ],
        compiler_params=pltpu.CompilerParams(collective_id=0, has_side_effects=True),
    )(
        velocity.reshape(3, rows, LANES),
        pressure.reshape(rows, LANES),
        pack(fields),
        pack(brownian),
    )
    unpacked = new_fields.reshape(3, count, rows, depth, LANES).transpose(0, 1, 3, 2, 4)
    return (
        unpacked.reshape(3, count, depth, extent),
        new_velocity.reshape(3, 1, extent),
    )


def solution(mesh):
    placed = (
        P(None, ("mesh", "field"), None),
        P(("mesh", "field"), None),
        P(None, "field", "mesh", None),
        P(None, "field", "mesh", None),
    )
    return jax.shard_map(
        functools.partial(body, mesh.shape["mesh"], mesh.shape["field"]),
        mesh=mesh,
        in_specs=placed,
        out_specs=(P(None, "field", "mesh", None), P(None, ("mesh", "field"), None)),
        check_vma=False,
    )
```

```python
import functools

import jax
import jax.numpy as jnp
from jax import lax
from jax.experimental import pallas as pl
from jax.experimental.pallas import tpu as pltpu
from jax.sharding import PartitionSpec as P

NY = 32
NZ = 32
SWEEPS = 4
LANES = 128
CHUNKS = 4
VMEM_LIMIT = 24 * 1024 * 1024

time_step = 0.02
axial_weight = 400.0
transverse_weight = 40.0
weissenberg = 0.5
max_stretch = 50.0
polymer_viscosity = 40.0
noise_scale = (0.02 / 0.5) ** 0.5
diagonal_weight = 1.0 / 0.02 + 2.0 * 400.0 + 4.0 * 40.0
index_table = ((0, 1, 2), (1, 3, 4), (2, 4, 5))
component_pairs = ((0, 0), (0, 1), (0, 2), (1, 1), (1, 2), (2, 2))
diagonal_pairs = (0, 3, 5)


def plane_shifts(x):
    rows = x.shape[0]
    lane = lax.broadcasted_iota(jnp.int32, x.shape, 1)
    row = lax.broadcasted_iota(jnp.int32, x.shape, 0)
    column = lane % NZ
    ahead = pltpu.roll(x, LANES - NZ, 1)
    ahead_next = jnp.where(row == rows - 1, 0.0, pltpu.roll(ahead, rows - 1, 0))
    y_plus = jnp.where(lane >= LANES - NZ, ahead_next, ahead)
    behind = pltpu.roll(x, NZ, 1)
    behind_next = jnp.where(row == 0, 0.0, pltpu.roll(behind, 1, 0))
    y_minus = jnp.where(lane < NZ, behind_next, behind)
    z_plus = jnp.where(column < NZ - 1, pltpu.roll(x, LANES - 1, 1), 0.0)
    z_minus = jnp.where(column > 0, pltpu.roll(x, 1, 1), 0.0)
    return y_plus, y_minus, z_plus, z_minus


def step_kernel(
    subdomains, groups,
    vel, prs, fld, brn, advanced, out_base, out_flow, out_stress,
    cur, noise, base, grads, sums, vp, parts, got, stress,
    load_sem, flow_sem, vp_send, vp_recv, part_send, part_recv, st_send, st_recv,
):
    total = subdomains * groups
    halo = SWEEPS
    width = max(halo, groups)
    rows = vel.shape[1]
    count = fld.shape[1]
    packed = fld.shape[2]
    block = min(16, packed)
    chunk = count // CHUNKS
    sub = lax.axis_index("mesh")
    own = lax.axis_index("field")
    plane = sub * groups + own
    offsets = [d for d in range(-width, width + 1) if d != 0]

    def inside(d):
        return (plane + d >= 0) & (plane + d < total)

    def device(d):
        return ((plane + d) // groups, (plane + d) % groups)

    flow_loads = [
        pltpu.make_async_copy(vel, vp.at[width, pl.ds(0, 3)], flow_sem.at[0]),
        pltpu.make_async_copy(prs, vp.at[width, 3], flow_sem.at[1]),
    ]
    for copy in flow_loads:
        copy.start()
    barrier = pltpu.get_barrier_semaphore()
    partners = jnp.int32(0)
    for d in offsets:
        @pl.when(inside(d))
        def _(d=d):
            pl.semaphore_signal(
                barrier, inc=1, device_id=device(d), device_id_type=pl.DeviceIdType.MESH
            )
        partners = partners + jnp.where(inside(d), 1, 0)
    loads = []
    for number in range(CHUNKS):
        part = pl.ds(number * chunk, chunk)
        loads.append((
            pltpu.make_async_copy(fld.at[:, part], cur.at[:, part], load_sem.at[0, number]),
            pltpu.make_async_copy(brn.at[:, part], noise.at[:, part], load_sem.at[1, number]),
        ))
        for copy in loads[-1]:
            copy.start()
    for d in offsets:
        @pl.when(jnp.logical_not(inside(d)))
        def _(d=d):
            vp[width + d] = jnp.zeros(vp.shape[1:], jnp.float32)
            stress[width + d] = jnp.zeros(stress.shape[1:], jnp.float32)
    for copy in flow_loads:
        copy.wait()
    pl.semaphore_wait(barrier, partners)

    def flow_copy(d):
        return pltpu.make_async_remote_copy(
            src_ref=vp.at[width], dst_ref=vp.at[width - d],
            send_sem=vp_send.at[width + d], recv_sem=vp_recv.at[width - d],
            device_id=device(d), device_id_type=pl.DeviceIdType.MESH,
        )

    for d in offsets:
        @pl.when(inside(d))
        def _(d=d):
            flow_copy(d).start()

    relax = time_step * max_stretch / (2.0 * weissenberg)
    for number in range(CHUNKS):
        for copy in loads[number]:
            copy.wait()

        @pl.loop(number * chunk, (number + 1) * chunk, unroll=2)
        def _(n):
            for start in range(0, packed, block):
                at = pl.ds(start, block)
                now = [cur[c, n, at].astype(jnp.float32) for c in range(3)]
                square = now[0] * now[0] + now[1] * now[1] + now[2] * now[2]
                keep = 1.0 - relax * (1.0 / (max_stretch - square))
                for c in range(3):
                    base[c, n, at] = now[c] * keep + noise_scale * noise[c, n, at].astype(jnp.float32)

    def wait_flow(slot):
        pltpu.make_async_copy(vp.at[width], vp.at[slot], vp_recv.at[slot]).wait()

    for q in range(-1, groups + 1):
        d = q - own
        @pl.when((d != 0) & inside(d))
        def _(d=d):
            wait_flow(width + d)
    for q in range(groups):
        here = width + q - own
        at = pl.ds(q, rows, stride=groups)
        for a in range(3):
            centre = vp[here, a]
            y_plus, y_minus, z_plus, z_minus = plane_shifts(centre)
            scale = 0.5 * time_step
            grads[3 * a, at] = (vp[here + 1, a] - vp[here - 1, a]) * scale
            grads[3 * a + 1, at] = (y_plus - y_minus) * scale
            grads[3 * a + 2, at] = (z_plus - z_minus) * scale

    for start in range(0, packed, block):
        at = pl.ds(start, block)
        g = [grads[k, at] for k in range(9)]

        def one_field(n, acc):
            now = [cur[c, n, at].astype(jnp.float32) for c in range(3)]
            new = []
            for a in range(3):
                value = base[a, n, at] + (
                    g[3 * a] * now[0] + g[3 * a + 1] * now[1] + g[3 * a + 2] * now[2]
                )
                advanced[a, n, at] = value.astype(jnp.bfloat16)
                new.append(value)
            square = new[0] * new[0] + new[1] * new[1] + new[2] * new[2]
            inverse = 1.0 / (max_stretch - square)
            pulled = [inverse * value for value in new]
            return tuple(
                total_k + pulled[left] * new[right]
                for total_k, (left, right) in zip(acc, component_pairs)
            )

        zero = jnp.zeros((block, LANES), jnp.float32)
        acc = lax.fori_loop(0, count, one_field, (zero,) * 6, unroll=2)
        for k in range(6):
            sums[k, at] = acc[k]

    for q in range(groups):
        for k in range(6):
            parts[q, k] = sums[k, pl.ds(q, rows, stride=groups)]

    def part_copy(r):
        to = (own + r) % groups
        return pltpu.make_async_remote_copy(
            src_ref=parts.at[to], dst_ref=got.at[r - 1],
            send_sem=part_send.at[r - 1], recv_sem=part_recv.at[r - 1],
            device_id=(sub, to), device_id_type=pl.DeviceIdType.MESH,
        )

    for r in range(1, groups):
        part_copy(r).start()

    for d in offsets:
        q = own + d
        @pl.when(inside(d) & ((q < -1) | (q > groups)))
        def _(d=d):
            wait_flow(width + d)
    reach = halo - 1
    for d in range(-halo, halo + 1):
        out_flow[halo + d] = vp[width + d, pl.ds(0, 3)]
    for d in range(-reach, reach + 1):
        here = width + d
        y_plus, y_minus, z_plus, z_minus = plane_shifts(vp[here, 3])
        slopes = (vp[here + 1, 3] - vp[here - 1, 3], y_plus - y_minus, z_plus - z_minus)
        for a in range(3):
            out_base[reach + d, a] = vp[here, a] * (1.0 / time_step) - 0.5 * slopes[a]

    for r in range(1, groups):
        part_copy(r).wait_recv()
    factor = polymer_viscosity / weissenberg
    for k in range(6):
        summed = parts[own, k]
        for r in range(1, groups):
            summed = summed + got[r - 1, k]
        value = summed * (factor * max_stretch / (count * groups))
        stress[width, k] = value - factor if k in diagonal_pairs else value

    def stress_copy(d):
        parts_of = pl.ds(0, 3 if abs(d) == halo else 6)
        return pltpu.make_async_remote_copy(
            src_ref=stress.at[width, parts_of], dst_ref=stress.at[width - d, parts_of],
            send_sem=st_send.at[width + d], recv_sem=st_recv.at[width - d],
            device_id=device(d), device_id_type=pl.DeviceIdType.MESH,
        )

    near = [d for d in offsets if abs(d) <= halo]
    for d in sorted(near, key=abs):
        @pl.when(inside(d))
        def _(d=d):
            stress_copy(d).start()
    for d in sorted(near, key=abs):
        @pl.when(inside(d))
        def _(d=d):
            stress_copy(-d).wait_recv()

    for d in range(-halo, halo + 1):
        out_stress[halo + d] = stress[width + d]

    for d in offsets:
        @pl.when(inside(d))
        def _(d=d):
            flow_copy(d).wait_send()
            if abs(d) <= halo:
                stress_copy(d).wait_send()
    for r in range(1, groups):
        part_copy(r).wait_send()


def momentum_kernel(
    subdomains, groups, advanced, source_base, flow, stress, out_fields, out_vel, vout, out_sem
):
    write = pltpu.make_async_copy(advanced, out_fields, out_sem.at[0])
    write.start()
    total = subdomains * groups
    halo = SWEEPS
    reach = halo - 1
    rows = flow.shape[2]
    plane = lax.axis_index("mesh") * groups + lax.axis_index("field")
    across = (
        lax.broadcasted_iota(jnp.int32, (rows, LANES), 0) * (LANES // NZ)
        + lax.broadcasted_iota(jnp.int32, (rows, LANES), 1) // NZ
    )
    solid = jnp.where((across < NY // 4) | (across >= NY - NY // 4), 1.0, 0.0)
    sources = {}
    fluid = {}
    for d in range(-reach, reach + 1):
        here = halo + d
        exists = jnp.where((plane + d >= 0) & (plane + d < total), 1.0 / diagonal_weight, 0.0)
        narrow = jnp.where(plane + d >= total // 2, 1.0, 0.0)
        fluid[d] = exists * (1.0 - narrow * solid)
        along_y = {}
        along_z = {}
        for k in range(1, 6):
            y_plus, y_minus, z_plus, z_minus = plane_shifts(stress[here, k])
            along_y[k] = y_plus - y_minus
            along_z[k] = z_plus - z_minus
        sources[d] = []
        for a in range(3):
            along_x = stress[here + 1, a] - stress[here - 1, a]
            slope = along_x + along_y[index_table[a][1]] + along_z[index_table[a][2]]
            sources[d].append(source_base[reach + d, a] + 0.5 * slope)

    for a in range(3):
        v = {d: flow[halo + d, a] for d in range(-halo, halo + 1)}
        for sweep in range(1, SWEEPS + 1):
            left = halo - sweep
            fresh = {}
            for d in range(-left, left + 1):
                y_plus, y_minus, z_plus, z_minus = plane_shifts(v[d])
                fresh[d] = fluid[d] * (
                    sources[d][a]
                    + axial_weight * (v[d + 1] + v[d - 1])
                    + transverse_weight * ((y_plus + y_minus) + (z_plus + z_minus))
                )
            v = fresh
        vout[a] = v[0]
    last = pltpu.make_async_copy(vout, out_vel, out_sem.at[1])
    last.start()
    write.wait()
    last.wait()


def body(subdomains, groups, velocity, pressure, fields, brownian):
    extent = velocity.shape[2]
    count, depth = fields.shape[1], fields.shape[2]
    rows = extent // LANES
    packed = rows * depth
    width = max(SWEEPS, groups)

    def pack(values):
        split = values.reshape(3, count, depth, rows, LANES)
        return split.transpose(0, 1, 3, 2, 4).reshape(3, count, packed, LANES)

    dma = pltpu.SemaphoreType.DMA
    near = pl.BlockSpec(memory_space=pltpu.VMEM)
    between = pl.pallas_call(
        functools.partial(step_kernel, subdomains, groups),
        out_shape=(
            pltpu.VMEM((3, count, packed, LANES), jnp.bfloat16),
            pltpu.VMEM((2 * SWEEPS - 1, 3, rows, LANES), jnp.float32),
            pltpu.VMEM((2 * SWEEPS + 1, 3, rows, LANES), jnp.float32),
            pltpu.VMEM((2 * SWEEPS + 1, 6, rows, LANES), jnp.float32),
        ),
        in_specs=[pl.BlockSpec(memory_space=pltpu.HBM)] * 4,
        out_specs=(near,) * 4,
        scratch_shapes=[
            pltpu.VMEM((3, count, packed, LANES), jnp.bfloat16),
            pltpu.VMEM((3, count, packed, LANES), jnp.bfloat16),
            pltpu.VMEM((3, count, packed, LANES), jnp.float32),
            pltpu.VMEM((9, packed, LANES), jnp.float32),
            pltpu.VMEM((6, packed, LANES), jnp.float32),
            pltpu.VMEM((2 * width + 1, 4, rows, LANES), jnp.float32),
            pltpu.VMEM((groups, 6, rows, LANES), jnp.float32),
            pltpu.VMEM((groups - 1, 6, rows, LANES), jnp.float32),
            pltpu.VMEM((2 * width + 1, 6, rows, LANES), jnp.float32),
            dma((2, CHUNKS)),
            dma((2,)),
            dma((2 * width + 1,)),
            dma((2 * width + 1,)),
            dma((groups - 1,)),
            dma((groups - 1,)),
            dma((2 * width + 1,)),
            dma((2 * width + 1,)),
        ],
        compiler_params=pltpu.CompilerParams(
            collective_id=0, has_side_effects=True, vmem_limit_bytes=VMEM_LIMIT
        ),
    )(
        *(
            pltpu.with_memory_space_constraint(values, pltpu.HBM)
            for values in (
                velocity.reshape(3, rows, LANES),
                pressure.reshape(rows, LANES),
                pack(fields),
                pack(brownian),
            )
        )
    )
    new_fields, new_velocity = pl.pallas_call(
        functools.partial(momentum_kernel, subdomains, groups),
        out_shape=(
            jax.ShapeDtypeStruct((3, count, packed, LANES), jnp.bfloat16),
            jax.ShapeDtypeStruct((3, rows, LANES), jnp.float32),
        ),
        in_specs=[near] * 4,
        out_specs=(pl.BlockSpec(memory_space=pltpu.HBM),) * 2,
        scratch_shapes=[pltpu.VMEM((3, rows, LANES), jnp.float32), dma((2,))],
        compiler_params=pltpu.CompilerParams(vmem_limit_bytes=VMEM_LIMIT),
    )(*between)
    unpacked = new_fields.reshape(3, count, rows, depth, LANES).transpose(0, 1, 3, 2, 4)
    return (
        unpacked.reshape(3, count, depth, extent),
        new_velocity.reshape(3, 1, extent),
    )


def solution(mesh):
    placed = (
        P(None, ("mesh", "field"), None),
        P(("mesh", "field"), None),
        P(None, "field", "mesh", None),
        P(None, "field", "mesh", None),
    )
    return jax.shard_map(
        functools.partial(body, mesh.shape["mesh"], mesh.shape["field"]),
        mesh=mesh,
        in_specs=placed,
        out_specs=(P(None, "field", "mesh", None), P(None, ("mesh", "field"), None)),
        check_vma=False,
    )
```

```python
import functools

import jax
import jax.numpy as jnp
from jax import lax
from jax.experimental import pallas as pl
from jax.experimental.pallas import tpu as pltpu
from jax.sharding import PartitionSpec as P

NY = 32
NZ = 32
SWEEPS = 4
LANES = 128
CHUNKS = 4
VMEM_LIMIT = 24 * 1024 * 1024

time_step = 0.02
axial_weight = 400.0
transverse_weight = 40.0
weissenberg = 0.5
max_stretch = 50.0
polymer_viscosity = 40.0
noise_scale = (0.02 / 0.5) ** 0.5
diagonal_weight = 1.0 / 0.02 + 2.0 * 400.0 + 4.0 * 40.0
index_table = ((0, 1, 2), (1, 3, 4), (2, 4, 5))
component_pairs = ((0, 0), (0, 1), (0, 2), (1, 1), (1, 2), (2, 2))
diagonal_pairs = (0, 3, 5)


def plane_shifts(x):
    rows = x.shape[0]
    lane = lax.broadcasted_iota(jnp.int32, x.shape, 1)
    row = lax.broadcasted_iota(jnp.int32, x.shape, 0)
    column = lane % NZ
    ahead = pltpu.roll(x, LANES - NZ, 1)
    ahead_next = jnp.where(row == rows - 1, 0.0, pltpu.roll(ahead, rows - 1, 0))
    y_plus = jnp.where(lane >= LANES - NZ, ahead_next, ahead)
    behind = pltpu.roll(x, NZ, 1)
    behind_next = jnp.where(row == 0, 0.0, pltpu.roll(behind, 1, 0))
    y_minus = jnp.where(lane < NZ, behind_next, behind)
    z_plus = jnp.where(column < NZ - 1, pltpu.roll(x, LANES - 1, 1), 0.0)
    z_minus = jnp.where(column > 0, pltpu.roll(x, 1, 1), 0.0)
    return y_plus, y_minus, z_plus, z_minus


def step_kernel(
    subdomains, groups,
    vel, prs, fld, brn, advanced, out_base, out_flow, out_stress,
    cur, noise, base, grads, sums, vp, parts, got, stress,
    load_sem, flow_sem, vp_send, vp_recv, part_send, part_recv, st_send, st_recv,
):
    total = subdomains * groups
    halo = SWEEPS
    width = max(halo, groups)
    rows = vel.shape[1]
    count = fld.shape[1]
    packed = fld.shape[2]
    block = min(16, packed)
    chunk = count // CHUNKS
    sub = lax.axis_index("mesh")
    own = lax.axis_index("field")
    plane = sub * groups + own
    offsets = [d for d in range(-width, width + 1) if d != 0]

    def inside(d):
        return (plane + d >= 0) & (plane + d < total)

    def device(d):
        return ((plane + d) // groups, (plane + d) % groups)

    flow_loads = [
        pltpu.make_async_copy(vel, vp.at[width, pl.ds(0, 3)], flow_sem.at[0]),
        pltpu.make_async_copy(prs, vp.at[width, 3], flow_sem.at[1]),
    ]
    for copy in flow_loads:
        copy.start()
    barrier = pltpu.get_barrier_semaphore()
    partners = jnp.int32(0)
    for d in offsets:
        @pl.when(inside(d))
        def _(d=d):
            pl.semaphore_signal(
                barrier, inc=1, device_id=device(d), device_id_type=pl.DeviceIdType.MESH
            )
        partners = partners + jnp.where(inside(d), 1, 0)
    loads = []
    for number in range(CHUNKS):
        part = pl.ds(number * chunk, chunk)
        loads.append((
            pltpu.make_async_copy(fld.at[:, part], cur.at[:, part], load_sem.at[0, number]),
            pltpu.make_async_copy(brn.at[:, part], noise.at[:, part], load_sem.at[1, number]),
        ))
        for copy in loads[-1]:
            copy.start()
    for d in offsets:
        @pl.when(jnp.logical_not(inside(d)))
        def _(d=d):
            vp[width + d] = jnp.zeros(vp.shape[1:], jnp.float32)
            stress[width + d] = jnp.zeros(stress.shape[1:], jnp.float32)
    for copy in flow_loads:
        copy.wait()
    pl.semaphore_wait(barrier, partners)

    def flow_copy(d):
        return pltpu.make_async_remote_copy(
            src_ref=vp.at[width], dst_ref=vp.at[width - d],
            send_sem=vp_send.at[width + d], recv_sem=vp_recv.at[width - d],
            device_id=device(d), device_id_type=pl.DeviceIdType.MESH,
        )

    def urgent(d):
        ahead = (plane + d) // groups - sub
        return (
            (ahead == 0)
            | ((ahead == 1) & (own == groups - 1))
            | ((ahead == -1) & (own == 0))
        )

    for d in sorted(offsets, key=abs):
        @pl.when(inside(d) & urgent(d))
        def _(d=d):
            flow_copy(d).start()

    relax = time_step * max_stretch / (2.0 * weissenberg)
    for number in range(CHUNKS):
        for copy in loads[number]:
            copy.wait()

        @pl.loop(number * chunk, (number + 1) * chunk, unroll=2)
        def _(n):
            for start in range(0, packed, block):
                at = pl.ds(start, block)
                now = [cur[c, n, at].astype(jnp.float32) for c in range(3)]
                square = now[0] * now[0] + now[1] * now[1] + now[2] * now[2]
                keep = 1.0 - relax * (1.0 / (max_stretch - square))
                for c in range(3):
                    base[c, n, at] = now[c] * keep + noise_scale * noise[c, n, at].astype(jnp.float32)

    for d in sorted(offsets, key=abs):
        @pl.when(inside(d) & jnp.logical_not(urgent(d)))
        def _(d=d):
            flow_copy(d).start()

    def wait_flow(slot):
        pltpu.make_async_copy(vp.at[width], vp.at[slot], vp_recv.at[slot]).wait()

    for q in range(-1, groups + 1):
        d = q - own
        @pl.when((d != 0) & inside(d))
        def _(d=d):
            wait_flow(width + d)
    for q in range(groups):
        here = width + q - own
        at = pl.ds(q, rows, stride=groups)
        for a in range(3):
            centre = vp[here, a]
            y_plus, y_minus, z_plus, z_minus = plane_shifts(centre)
            scale = 0.5 * time_step
            grads[3 * a, at] = (vp[here + 1, a] - vp[here - 1, a]) * scale
            grads[3 * a + 1, at] = (y_plus - y_minus) * scale
            grads[3 * a + 2, at] = (z_plus - z_minus) * scale

    blocks = packed // block
    piece = block // groups

    def part_copy(number, r):
        to = (own + r) % groups
        return pltpu.make_async_remote_copy(
            src_ref=parts.at[number, to], dst_ref=got.at[number, r - 1],
            send_sem=part_send.at[number, r - 1], recv_sem=part_recv.at[number, r - 1],
            device_id=(sub, to), device_id_type=pl.DeviceIdType.MESH,
        )

    for start in range(0, packed, block):
        at = pl.ds(start, block)
        g = [grads[k, at] for k in range(9)]

        def one_field(n, acc):
            now = [cur[c, n, at].astype(jnp.float32) for c in range(3)]
            new = []
            for a in range(3):
                value = base[a, n, at] + (
                    g[3 * a] * now[0] + g[3 * a + 1] * now[1] + g[3 * a + 2] * now[2]
                )
                advanced[a, n, at] = value.astype(jnp.bfloat16)
                new.append(value)
            square = new[0] * new[0] + new[1] * new[1] + new[2] * new[2]
            inverse = 1.0 / (max_stretch - square)
            pulled = [inverse * value for value in new]
            return tuple(
                total_k + pulled[left] * new[right]
                for total_k, (left, right) in zip(acc, component_pairs)
            )

        zero = jnp.zeros((block, LANES), jnp.float32)
        acc = lax.fori_loop(0, count, one_field, (zero,) * 6, unroll=2)
        for k in range(6):
            sums[k, at] = acc[k]

        number = start // block
        for q in range(groups):
            for k in range(6):
                parts[number, q, pl.ds(k * piece, piece)] = sums[
                    k, pl.ds(start + q, piece, stride=groups)
                ]
        for r in range(1, groups):
            part_copy(number, r).start()

    for d in offsets:
        q = own + d
        @pl.when(inside(d) & ((q < -1) | (q > groups)))
        def _(d=d):
            wait_flow(width + d)
    reach = halo - 1
    for d in range(-halo, halo + 1):
        out_flow[halo + d] = vp[width + d, pl.ds(0, 3)]
    for d in range(-reach, reach + 1):
        here = width + d
        y_plus, y_minus, z_plus, z_minus = plane_shifts(vp[here, 3])
        slopes = (vp[here + 1, 3] - vp[here - 1, 3], y_plus - y_minus, z_plus - z_minus)
        for a in range(3):
            out_base[reach + d, a] = vp[here, a] * (1.0 / time_step) - 0.5 * slopes[a]

    factor = polymer_viscosity / weissenberg
    for number in range(blocks):
        summed = parts[number, own]
        for r in range(1, groups):
            part_copy(number, r).wait_recv()
            summed = summed + got[number, r - 1]
        value = summed * (factor * max_stretch / (count * groups))
        for k in range(6):
            of_pair = value[k * piece : (k + 1) * piece]
            if k in diagonal_pairs:
                of_pair = of_pair - factor
            stress[width, k, pl.ds(number * piece, piece)] = of_pair

    def stress_copy(d):
        parts_of = pl.ds(0, 3 if abs(d) == halo else 6)
        return pltpu.make_async_remote_copy(
            src_ref=stress.at[width, parts_of], dst_ref=stress.at[width - d, parts_of],
            send_sem=st_send.at[width + d], recv_sem=st_recv.at[width - d],
            device_id=device(d), device_id_type=pl.DeviceIdType.MESH,
        )

    near = [d for d in offsets if abs(d) <= halo]
    for d in sorted(near, key=abs):
        @pl.when(inside(d))
        def _(d=d):
            stress_copy(d).start()
    for d in sorted(near, key=abs):
        @pl.when(inside(d))
        def _(d=d):
            stress_copy(-d).wait_recv()

    for d in range(-halo, halo + 1):
        out_stress[halo + d] = stress[width + d]

    for d in offsets:
        @pl.when(inside(d))
        def _(d=d):
            flow_copy(d).wait_send()
            if abs(d) <= halo:
                stress_copy(d).wait_send()
    for number in range(blocks):
        for r in range(1, groups):
            part_copy(number, r).wait_send()


def momentum_kernel(
    subdomains, groups, advanced, source_base, flow, stress, out_fields, out_vel, vout, out_sem
):
    write = pltpu.make_async_copy(advanced, out_fields, out_sem.at[0])
    write.start()
    total = subdomains * groups
    halo = SWEEPS
    reach = halo - 1
    rows = flow.shape[2]
    plane = lax.axis_index("mesh") * groups + lax.axis_index("field")
    across = (
        lax.broadcasted_iota(jnp.int32, (rows, LANES), 0) * (LANES // NZ)
        + lax.broadcasted_iota(jnp.int32, (rows, LANES), 1) // NZ
    )
    solid = jnp.where((across < NY // 4) | (across >= NY - NY // 4), 1.0, 0.0)
    sources = {}
    fluid = {}
    for d in range(-reach, reach + 1):
        here = halo + d
        exists = jnp.where((plane + d >= 0) & (plane + d < total), 1.0 / diagonal_weight, 0.0)
        narrow = jnp.where(plane + d >= total // 2, 1.0, 0.0)
        fluid[d] = exists * (1.0 - narrow * solid)
        along_y = {}
        along_z = {}
        for k in range(1, 6):
            y_plus, y_minus, z_plus, z_minus = plane_shifts(stress[here, k])
            along_y[k] = y_plus - y_minus
            along_z[k] = z_plus - z_minus
        sources[d] = []
        for a in range(3):
            along_x = stress[here + 1, a] - stress[here - 1, a]
            slope = along_x + along_y[index_table[a][1]] + along_z[index_table[a][2]]
            sources[d].append(source_base[reach + d, a] + 0.5 * slope)

    for a in range(3):
        v = {d: flow[halo + d, a] for d in range(-halo, halo + 1)}
        for sweep in range(1, SWEEPS + 1):
            left = halo - sweep
            fresh = {}
            for d in range(-left, left + 1):
                y_plus, y_minus, z_plus, z_minus = plane_shifts(v[d])
                fresh[d] = fluid[d] * (
                    sources[d][a]
                    + axial_weight * (v[d + 1] + v[d - 1])
                    + transverse_weight * ((y_plus + y_minus) + (z_plus + z_minus))
                )
            v = fresh
        vout[a] = v[0]
    last = pltpu.make_async_copy(vout, out_vel, out_sem.at[1])
    last.start()
    write.wait()
    last.wait()


def body(subdomains, groups, velocity, pressure, fields, brownian):
    extent = velocity.shape[2]
    count, depth = fields.shape[1], fields.shape[2]
    rows = extent // LANES
    packed = rows * depth
    blocks = packed // min(16, packed)
    width = max(SWEEPS, groups)

    def pack(values):
        split = values.reshape(3, count, depth, rows, LANES)
        return split.transpose(0, 1, 3, 2, 4).reshape(3, count, packed, LANES)

    dma = pltpu.SemaphoreType.DMA
    near = pl.BlockSpec(memory_space=pltpu.VMEM)
    between = pl.pallas_call(
        functools.partial(step_kernel, subdomains, groups),
        out_shape=(
            pltpu.VMEM((3, count, packed, LANES), jnp.bfloat16),
            pltpu.VMEM((2 * SWEEPS - 1, 3, rows, LANES), jnp.float32),
            pltpu.VMEM((2 * SWEEPS + 1, 3, rows, LANES), jnp.float32),
            pltpu.VMEM((2 * SWEEPS + 1, 6, rows, LANES), jnp.float32),
        ),
        in_specs=[pl.BlockSpec(memory_space=pltpu.HBM)] * 4,
        out_specs=(near,) * 4,
        scratch_shapes=[
            pltpu.VMEM((3, count, packed, LANES), jnp.bfloat16),
            pltpu.VMEM((3, count, packed, LANES), jnp.bfloat16),
            pltpu.VMEM((3, count, packed, LANES), jnp.float32),
            pltpu.VMEM((9, packed, LANES), jnp.float32),
            pltpu.VMEM((6, packed, LANES), jnp.float32),
            pltpu.VMEM((2 * width + 1, 4, rows, LANES), jnp.float32),
            pltpu.VMEM((blocks, groups, 6 * rows // blocks, LANES), jnp.float32),
            pltpu.VMEM((blocks, groups - 1, 6 * rows // blocks, LANES), jnp.float32),
            pltpu.VMEM((2 * width + 1, 6, rows, LANES), jnp.float32),
            dma((2, CHUNKS)),
            dma((2,)),
            dma((2 * width + 1,)),
            dma((2 * width + 1,)),
            dma((blocks, groups - 1)),
            dma((blocks, groups - 1)),
            dma((2 * width + 1,)),
            dma((2 * width + 1,)),
        ],
        compiler_params=pltpu.CompilerParams(
            collective_id=0, has_side_effects=True, vmem_limit_bytes=VMEM_LIMIT
        ),
    )(
        *(
            pltpu.with_memory_space_constraint(values, pltpu.HBM)
            for values in (
                velocity.reshape(3, rows, LANES),
                pressure.reshape(rows, LANES),
                pack(fields),
                pack(brownian),
            )
        )
    )
    new_fields, new_velocity = pl.pallas_call(
        functools.partial(momentum_kernel, subdomains, groups),
        out_shape=(
            jax.ShapeDtypeStruct((3, count, packed, LANES), jnp.bfloat16),
            jax.ShapeDtypeStruct((3, rows, LANES), jnp.float32),
        ),
        in_specs=[near] * 4,
        out_specs=(pl.BlockSpec(memory_space=pltpu.HBM),) * 2,
        scratch_shapes=[pltpu.VMEM((3, rows, LANES), jnp.float32), dma((2,))],
        compiler_params=pltpu.CompilerParams(vmem_limit_bytes=VMEM_LIMIT),
    )(*between)
    unpacked = new_fields.reshape(3, count, rows, depth, LANES).transpose(0, 1, 3, 2, 4)
    return (
        unpacked.reshape(3, count, depth, extent),
        new_velocity.reshape(3, 1, extent),
    )


def solution(mesh):
    placed = (
        P(None, ("mesh", "field"), None),
        P(("mesh", "field"), None),
        P(None, "field", "mesh", None),
        P(None, "field", "mesh", None),
    )
    return jax.shard_map(
        functools.partial(body, mesh.shape["mesh"], mesh.shape["field"]),
        mesh=mesh,
        in_specs=placed,
        out_specs=(P(None, "field", "mesh", None), P(None, ("mesh", "field"), None)),
        check_vma=False,
    )
```
